128 devices in a mesh: seq: 16 (over x, y), head: 8 (over z, core).
Axes of the slice: x: 4, y: 4, z: 4, core: 2. Of those that a mesh axis runs over, the one named last changes fastest.
Arguments:
- queries: bfloat16 [4096, 12288], P('seq', 'head'), may hold values from -256 to 256
- own_latent: bfloat16 [4096, 576], P('seq'), may hold values from -16 to 16
- cache: bfloat16 [512, 128, 576], P('seq', 'head'), may hold values from -6 to 6
- block_list: int32 [16, 32], replicated, may hold values from 0 to 511, as said below
- offsets: int32 [16, 32], P('seq'), may hold values from -4096 to 4096
- tile_mask: int32 [16, 2, 32], P('seq'), may hold values 0 or 1
- w_uk: bfloat16 [64, 128, 512], P('head'), may hold values from -0.5 to 0.5
- w_uv: bfloat16 [64, 512, 128], P('head'), may hold values from -0.25 to 0.25
- w_o: bfloat16 [8192, 7168], P('head'), may hold values from -0.0625 to 0.0625
Outputs:
- layer_out: bfloat16 [4096, 7168], P('seq', 'head')
The draws below stay inside these ranges and needn't reach their ends.
Inputs may be any that keep to these rules, and one draw needn't show every extreme that they name: `block_list`: entry (r, j) names a pooled span whose owner is index entry // 32 of seq. In each row no owner is named more than 4 times, and at least one owner is named exactly 4 times.
All inputs are finite; a program needn't handle non-finite values. No bound on the sum of `tile_mask` on one device may be relied on, other than what follows from the above.
Results may differ from the reference program's by a relative error of at most 0.015.
Values may be sent and summed in bfloat16 or wider, within the bound.
No kernel may reach another device: no remote copies, remote signals or barrier semaphores. Data moves between devices by JAX's collectives and lax.ppermute only.
A program may use at most 128 MiB of HBM per device.

```python
import jax
import jax.numpy as jnp
from jax import lax

D = 7168
HEADS = 64
NOPE = 128
ROPE = 64
V = 128
LAT = 512
SLAB = 256
SPAN_DEV = 32
SPAN = 128
LISTED = 32
MOST = 4
TOKENS = 4096
QTILES = 2
N_SEQ = 16
N_HEAD = 8


def drawn_pair(key):
    base = jax.random.fold_in(key, 4049)
    keys_list = jax.random.split(base, 3)
    latent = jnp.clip(jax.random.normal(keys_list[0], (TOKENS, LAT + ROPE), jnp.float32), -6.0, 6.0)
    nope_part = jnp.clip(jax.random.normal(keys_list[1], (TOKENS, HEADS, NOPE), jnp.float32), -6.0, 6.0)
    rope_query = jnp.clip(jax.random.normal(keys_list[2], (TOKENS, HEADS, ROPE), jnp.float32), -6.0, 6.0)
    query = jnp.concatenate([nope_part, rope_query], axis=2).reshape(TOKENS, HEADS * (NOPE + ROPE))
    return (jnp.clip(latent, -16.0, 16.0), jnp.clip(query, -256.0, 256.0))


def draw_queries(key, part):
    return drawn_pair(key)[1].astype(jnp.bfloat16)


def draw_own_latent(key, part):
    return drawn_pair(key)[0].astype(jnp.bfloat16)


def draw_block_list(key, part):
    base = jax.random.fold_in(key, 7)

    def one_row(row_key):
        key_owner, key_slots, key_order, key_span = jax.random.split(row_key, 4)
        leading = jax.random.randint(key_owner, (), 0, N_SEQ)
        slot_order = jax.random.permutation(key_slots, (N_SEQ - 1) * MOST)
        others = slot_order[:LISTED - MOST] // MOST
        others = others + (others >= leading).astype(jnp.int32)
        owners = jnp.concatenate([jnp.full((MOST,), leading, jnp.int32), others.astype(jnp.int32)])
        owners = jax.random.permutation(key_order, owners)
        within = jax.random.randint(key_span, (LISTED,), 0, SPAN_DEV)
        return (owners * SPAN_DEV + within).astype(jnp.int32)
    return jax.vmap(one_row)(jax.random.split(base, N_SEQ))


def plant(values, stream_key, smallest, top_value):
    extent = values.shape
    spot = [jax.random.randint(jax.random.fold_in(stream_key, axis), (), 0, extent[axis]) for axis in range(len(extent))]
    values = values.at[tuple(spot)].set(smallest)
    longest = extent.index(max(extent))
    spot[longest] = (spot[longest] + 1) % extent[longest]
    return values.at[tuple(spot)].set(top_value)


def shard_levels(key, shape, cuts, least, largest):
    factor_of = 1.0
    for dim, blocks in cuts:
        steps = jax.random.uniform(jax.random.fold_in(jax.random.fold_in(key, 6), dim), (blocks,), jnp.float32, least / len(cuts), largest / len(cuts))
        factor_of = factor_of * jnp.repeat(jnp.exp(steps), shape[dim] // blocks).reshape((-1,) + (1,) * (len(shape) - 1 - dim))
    return factor_of


def noise(own_key, shape, spread, most, shards=(), kind=jnp.bfloat16):
    values = spread * jax.random.normal(own_key, shape, jnp.float32)
    if shards:
        values = values * shard_levels(own_key, shape, shards, -0.22, 0.18)
    return jnp.clip(values, -most, most).astype(kind)


def setup_inputs(seed: int = 0) -> dict:
    arg_keys = jax.random.split(jax.random.key(seed), 10)
    return {
        "queries": draw_queries(jax.random.fold_in(arg_keys[9], 71), 0),
        "own_latent": draw_own_latent(jax.random.fold_in(arg_keys[9], 71), 0),
        "cache": noise(arg_keys[2], (SPAN_DEV * N_SEQ, SPAN, LAT + ROPE), 1.0, 6.0, ((0, 16), (1, 8))),
        "block_list": draw_block_list(jax.random.fold_in(arg_keys[9], 71), 0),
        "offsets": plant(jax.random.randint(arg_keys[4], (N_SEQ, LISTED), -4096, 4097), jax.random.fold_in(arg_keys[4], 1), -4096, 4096).astype(jnp.int32),
        "tile_mask": plant((jax.random.randint(arg_keys[5], (N_SEQ, QTILES, LISTED), 0, 5) < 3).astype(jnp.int32), jax.random.fold_in(arg_keys[5], 1), 0, 1),
        "w_uk": noise(arg_keys[6], (HEADS, NOPE, LAT), NOPE ** -0.5, 0.5, ((0, 8),)),
        "w_uv": noise(arg_keys[7], (HEADS, LAT, V), LAT ** -0.5, 0.25, ((0, 8),)),
        "w_o": noise(arg_keys[8], (HEADS * V, D), (HEADS * V) ** -0.5, 0.0625, ((0, 8),)),
    }


THETA = 50000.0


def rerotate(blocks, shift):
    halfway = ROPE // 2
    inverse = THETA ** (-jnp.arange(halfway, dtype=jnp.float32) * 2.0 / ROPE)
    angles = shift.astype(jnp.float32)[:, None] * inverse[None, :]
    cosine_table = jnp.cos(angles)[:, None, :]
    sine_table = jnp.sin(angles)[:, None, :]
    rotary = blocks[..., LAT:].astype(jnp.float32)
    first_half = rotary[..., :halfway]
    second_half = rotary[..., halfway:]
    turned = jnp.concatenate([first_half * cosine_table - second_half * sine_table, second_half * cosine_table + first_half * sine_table], axis=-1)
    return jnp.concatenate([blocks[..., :LAT], turned.astype(jnp.bfloat16)], axis=-1)


def allowed_keys(tiles, query_rows, block_rows):
    listed_mask = jnp.repeat(jnp.repeat(tiles > 0, block_rows, axis=0), block_rows, axis=1)
    causal = jnp.tril(jnp.ones((query_rows, query_rows), jnp.bool_))
    return jnp.concatenate([causal, listed_mask], axis=1)


def attend(grouped, context, allowed, key_maps, value_maps):
    nope_width = key_maps.shape[1]
    latent_width = key_maps.shape[2]
    factor = grouped.shape[-1] ** -0.5
    value_latent = context[:, :latent_width]

    def one_head(inputs):
        head_query, key_map, value_map = inputs
        query_latent = jnp.dot(head_query[:, :nope_width], key_map, preferred_element_type=jnp.float32).astype(jnp.bfloat16)
        query_full = jnp.concatenate([query_latent, head_query[:, nope_width:]], axis=1)
        scores = lax.dot_general(query_full, context, (((1,), (1,)), ((), ())), preferred_element_type=jnp.float32) * factor
        scores = jnp.where(allowed, scores, -1e30)
        highest = jnp.max(scores, axis=1, keepdims=True)
        weights = jnp.exp(scores - highest)
        denominator = jnp.sum(weights, axis=1, keepdims=True)
        shares = (weights / denominator).astype(jnp.bfloat16)
        mixed_latent = jnp.dot(shares, value_latent, preferred_element_type=jnp.float32).astype(jnp.bfloat16)
        return jnp.dot(mixed_latent, value_map, preferred_element_type=jnp.float32).astype(jnp.bfloat16)

    per_head = lax.map(one_head, (jnp.transpose(grouped, (1, 0, 2)), key_maps, value_maps))
    return jnp.transpose(per_head, (1, 0, 2)).reshape(grouped.shape[0], -1)


def reference(queries, own_latent, cache, block_list, offsets, tile_mask, w_uk, w_uv, w_o):
    slab_queries = queries.reshape(N_SEQ, SLAB, HEADS, NOPE + ROPE)
    slab_latent = own_latent.reshape(N_SEQ, SLAB, LAT + ROPE)

    def one_slab(inputs):
        grouped, own_rows, listing, shifts, tiles = inputs
        blocks = rerotate(cache[listing], shifts).reshape(LISTED * SPAN, LAT + ROPE)
        context = jnp.concatenate([own_rows, blocks], axis=0)
        allowed = allowed_keys(tiles, SLAB, SPAN)
        head_out = attend(grouped, context, allowed, w_uk, w_uv)
        split_out = head_out.reshape(SLAB, N_HEAD, -1).astype(jnp.float32)
        split_proj = w_o.reshape(N_HEAD, -1, D).astype(jnp.float32)
        partials = jnp.einsum("sgk,gkd->gsd", split_out, split_proj).astype(jnp.bfloat16)
        partials = lax.optimization_barrier(partials)
        return jnp.sum(partials.astype(jnp.float32), axis=0).astype(jnp.bfloat16)

    result = lax.map(one_slab, (slab_queries, slab_latent, block_list, offsets, tile_mask))
    return result.reshape(N_SEQ * SLAB, D)
```

```python
import functools

import jax
import jax.numpy as jnp
from jax import lax
from jax.experimental import pallas as pl
from jax.experimental.pallas import tpu as pltpu
from jax.sharding import Mesh, PartitionSpec as P

MOST = 4
THETA = 50000.0
TILE = 128
NEG = -1e30
VMEM = pltpu.VMEM
SMEM = pltpu.SMEM


def vspec():
    return pl.BlockSpec(memory_space=VMEM)


def sspec():
    return pl.BlockSpec(memory_space=SMEM)


def params(mib):
    return pltpu.CompilerParams(vmem_limit_bytes=mib * 1024 * 1024)


def dot_t(a, b):
    return lax.dot_general(a, b, (((1,), (1,)), ((), ())), preferred_element_type=jnp.float32)


def dot(a, b):
    return jnp.dot(a, b, preferred_element_type=jnp.float32)


def pick_kernel(slot_ref, arrived_ref, cos_ref, sin_ref, out_ref):
    latent = out_ref.shape[2] - 64
    for j in range(out_ref.shape[0]):
        rows = arrived_ref[slot_ref[j]]
        out_ref[j, :, :latent] = rows[:, :latent]
        rotary = rows[:, latent:].astype(jnp.float32)
        swapped = jnp.concatenate([rotary[:, 32:], rotary[:, :32]], axis=1)
        turned = rotary * cos_ref[j][None, :] + swapped * sin_ref[j][None, :]
        out_ref[j, :, latent:] = turned.astype(jnp.bfloat16)


def pick(slots, arrived, cosines, sines):
    count = slots.shape[0]
    return pl.pallas_call(
        pick_kernel,
        name="pick",
        out_shape=jax.ShapeDtypeStruct((count,) + arrived.shape[1:], jnp.bfloat16),
        in_specs=[sspec(), vspec(), vspec(), vspec()],
        out_specs=vspec(),
        compiler_params=params(16),
    )(slots, arrived, cosines, sines)


def fold(s, v, t, scale, high_ref, sum_ref, acc_ref):
    old = high_ref[t]
    new = jnp.maximum(old, jnp.max(s, axis=1, keepdims=True))
    alpha = jnp.exp((old - new) * scale)
    width = s.shape[1] // 128
    p = jnp.exp((s - jnp.concatenate([new] * width, axis=1)) * scale)
    part = p[:, :128]
    for w in range(1, width):
        part = part + p[:, w * 128 : (w + 1) * 128]
    sum_ref[t] = sum_ref[t] * alpha + part
    high_ref[t] = new
    wide = jnp.concatenate([alpha] * (acc_ref.shape[2] // 128), axis=1)
    acc_ref[t] = acc_ref[t] * wide + dot(p.astype(jnp.bfloat16), v)


def start_kernel(mask_ref, q_ref, own_ref, uk_ref, q_out, list_out, high_ref, sum_ref, acc_ref, *, scale):
    heads, nope, latent = uk_ref.shape
    rope = own_ref.shape[1] - latent
    width = nope + rope
    tiles = q_ref.shape[0] // TILE
    listed = mask_ref.shape[1]
    for t in range(tiles):
        for j in range(list_out.shape[1]):
            list_out[t, j] = 0
        count = jnp.int32(0)
        for j in range(listed):
            list_out[t, count] = j
            count = count + (mask_ref[t, j] > 0).astype(jnp.int32)
        list_out[t, list_out.shape[1] - 1] = count
    for h in range(heads):
        ql = dot(q_ref[:, h * width : h * width + nope], uk_ref[h]).astype(jnp.bfloat16)
        qr = q_ref[:, h * width + nope : (h + 1) * width]
        for t in range(tiles):
            q_out[t, h * TILE : (h + 1) * TILE, :latent] = ql[t * TILE : (t + 1) * TILE]
            q_out[t, h * TILE : (h + 1) * TILE, latent:] = qr[t * TILE : (t + 1) * TILE]
    rows = heads * TILE
    for t in range(tiles):
        keys = own_ref[: (t + 1) * TILE]
        s = dot_t(q_out[t], keys)
        row = lax.broadcasted_iota(jnp.int32, s.shape, 0) % TILE + t * TILE
        col = lax.broadcasted_iota(jnp.int32, s.shape, 1)
        s = jnp.where(col <= row, s, NEG)
        high = jnp.max(s, axis=1, keepdims=True)
        p = jnp.exp((s - high) * scale)
        part = p[:, :128]
        for w in range(1, t + 1):
            part = part + p[:, w * 128 : (w + 1) * 128]
        high_ref[t] = jnp.broadcast_to(high, (rows, 128))
        sum_ref[t] = part
        acc_ref[t] = dot(p.astype(jnp.bfloat16), keys[:, :latent])


def start(tile_mask, queries, own, w_uk, scale):
    tiles, listed = tile_mask.shape
    heads, nope, latent = w_uk.shape
    rows = heads * TILE
    f32 = jnp.float32
    return pl.pallas_call(
        functools.partial(start_kernel, scale=scale),
        name="start",
        out_shape=(
            jax.ShapeDtypeStruct((tiles, rows, own.shape[1]), jnp.bfloat16),
            jax.ShapeDtypeStruct((tiles, listed + 9), jnp.int32),
            jax.ShapeDtypeStruct((tiles, rows, 128), f32),
            jax.ShapeDtypeStruct((tiles, rows, 128), f32),
            jax.ShapeDtypeStruct((tiles, rows, latent), f32),
        ),
        in_specs=[sspec(), vspec(), vspec(), vspec()],
        out_specs=(vspec(), sspec(), vspec(), vspec(), vspec()),
        compiler_params=params(40),
    )(tile_mask, queries, own, w_uk)


def stage_kernel(list_ref, q_ref, *refs, pieces, scale, final):
    piece_refs = refs[:pieces]
    refs = refs[pieces:]
    if final:
        uv_ref, high_in, sum_in, acc_in, out_ref, high_ref, sum_ref, acc_ref = refs
    else:
        high_in, sum_in, acc_in, high_ref, sum_ref, acc_ref = refs
    high_ref[...] = high_in[...]
    sum_ref[...] = sum_in[...]
    acc_ref[...] = acc_in[...]
    latent = acc_ref.shape[2]
    tiles = q_ref.shape[0]
    per = pieces * piece_refs[0].shape[1]
    group = 256 // per
    last = list_ref.shape[1] - 1
    for t in range(tiles):
        count = list_ref[t, last]

        def body(g, carry, t=t, count=count):
            keys = jnp.concatenate(
                [ref[list_ref[t, g * group + i]] for i in range(group) for ref in piece_refs],
                axis=0,
            )
            s = dot_t(q_ref[t], keys)
            col = lax.broadcasted_iota(jnp.int32, s.shape, 1)
            s = jnp.where(col < (count - g * group) * per, s, NEG)
            fold(s, keys[:, :latent], t, scale, high_ref, sum_ref, acc_ref)
            return carry

        lax.fori_loop(0, (count + group - 1) // group, body, 0)
    if final:
        heads = uv_ref.shape[0]
        for t in range(tiles):
            total = jnp.sum(sum_ref[t], axis=1, keepdims=True)
            mixed = (acc_ref[t] / total).astype(jnp.bfloat16)
            for h in range(heads):
                out_ref[t * TILE : (t + 1) * TILE, h * 128 : (h + 1) * 128] = dot(
                    mixed[h * TILE : (h + 1) * TILE], uv_ref[h]
                ).astype(jnp.bfloat16)


def stage(lists, q, pieces, state, scale, w_uv=None):
    final = w_uv is not None
    tiles, rows, latent = state[2].shape
    f32 = jnp.float32
    shapes = tuple(jax.ShapeDtypeStruct(x.shape, x.dtype) for x in state)
    if final:
        out_shape = jax.ShapeDtypeStruct((tiles * TILE, w_uv.shape[0] * 128), jnp.bfloat16)
        scratch = [pltpu.VMEM(x.shape, x.dtype) for x in state]
        aliases = {}
        extra = (w_uv,)
        out_specs = vspec()
    else:
        out_shape = shapes
        scratch = []
        first = 2 + len(pieces)
        aliases = {first: 0, first + 1: 1, first + 2: 2}
        extra = ()
        out_specs = (vspec(),) * 3
    args = (lists, q, *pieces, *extra, *state)
    return pl.pallas_call(
        functools.partial(stage_kernel, pieces=len(pieces), scale=scale, final=final),
        name="stage",
        out_shape=out_shape,
        in_specs=[sspec()] + [vspec()] * (len(args) - 1),
        out_specs=out_specs,
        scratch_shapes=scratch,
        input_output_aliases=aliases,
        compiler_params=params(48),
    )(*args)


def per_device(queries, own_latent, cache, block_list, offsets, tile_mask, w_uk, w_uv, w_o):
    seq = ("x", "y")
    seq_count = lax.axis_size(seq)
    seq_index = lax.axis_index(seq)
    spans_held = cache.shape[0]
    latent_full = cache.shape[2]
    listed_count = block_list.shape[1]
    latent = w_uk.shape[2]
    rope = latent_full - latent
    width = w_uk.shape[1] + rope
    scale = width ** (-0.5)

    owners = block_list // spans_held
    within = block_list % spans_held
    earlier = jnp.tril(jnp.ones((listed_count, listed_count), jnp.bool_), -1)
    same_owner = owners[:, :, None] == owners[:, None, :]
    ranking = jnp.sum(same_owner & earlier[None], axis=2)
    slot_ids = jnp.arange(MOST, dtype=jnp.int32)
    matches = (owners == seq_index)[:, :, None] & (ranking[:, :, None] == slot_ids[None, None, :])
    send_index = jnp.sum(jnp.where(matches, within[:, :, None], 0), axis=1)
    my_owners = lax.dynamic_index_in_dim(owners, seq_index, 0, keepdims=False)
    my_ranking = lax.dynamic_index_in_dim(ranking, seq_index, 0, keepdims=False)
    flat_slot = my_owners * MOST + my_ranking
    arrived = lax.all_to_all(cache[send_index], seq, split_axis=0, concat_axis=0, tiled=True)

    inverse = THETA ** (-jnp.arange(rope // 2, dtype=jnp.float32) * 2.0 / rope)
    angles = offsets[0].astype(jnp.float32)[:, None] * inverse[None, :]
    cosine = jnp.cos(angles)
    sine = jnp.sin(angles)
    cosines = jnp.concatenate([cosine, cosine], axis=1)
    sines = jnp.concatenate([-sine, sine], axis=1)
    q, lists, high, total, acc = start(tile_mask[0], queries, own_latent, w_uk, scale)

    own = pick(
        flat_slot,
        arrived.reshape(seq_count * MOST, cache.shape[1], latent_full),
        cosines,
        sines,
    )
    size = lax.axis_size("z")
    up = [(i, (i + 1) % size) for i in range(size)]
    down = [(i, (i - 1) % size) for i in range(size)]
    swap = [(0, 1), (1, 0)]
    half = own.shape[0] // 2
    plus = lax.ppermute(own, "z", up)
    minus = lax.ppermute(own, "z", down)
    far = jnp.concatenate(
        [lax.ppermute(plus[:half], "z", up), lax.ppermute(minus[half:], "z", down)], axis=0
    )
    pieces = [own, plus, minus, far]
    pieces = pieces + [lax.ppermute(x, "c", swap) for x in pieces]
    head_out = stage(lists, q, pieces, (high, total, acc), scale, w_uv)

    features = w_o.shape[1] // (2 * size)
    partial = jnp.dot(head_out, w_o, preferred_element_type=jnp.float32)
    core = lax.axis_index("c")
    rows = partial.shape[0]
    split = partial.reshape(rows, size, 2, features)
    mine = lax.dynamic_index_in_dim(split, core, 2, keepdims=False)
    other = lax.dynamic_index_in_dim(split, 1 - core, 2, keepdims=False).astype(jnp.bfloat16)
    other = lax.ppermute(other, "c", swap)
    chip = mine.astype(jnp.bfloat16).astype(jnp.float32) + other.astype(jnp.float32)
    level = lax.axis_index("z")

    def part(k):
        return lax.dynamic_index_in_dim(chip, (level + k) % size, 1, keepdims=False)

    bf = jnp.bfloat16
    f32 = jnp.float32
    h = rows // 2
    far_sum = part(2).astype(bf)
    from_below = lax.ppermute(far_sum[:h], "z", up)
    from_above = lax.ppermute(far_sum[h:], "z", down)
    upward = part(1)
    upward = jnp.concatenate([upward[:h] + from_below.astype(f32), upward[h:]], axis=0).astype(bf)
    downward = part(3)
    downward = jnp.concatenate(
        [downward[:h], downward[h:] + from_above.astype(f32)], axis=0
    ).astype(bf)
    below = lax.ppermute(upward, "z", up)
    above = lax.ppermute(downward, "z", down)
    return (part(0) + below.astype(f32) + above.astype(f32)).astype(bf)


def solution(mesh):
    fine = Mesh(mesh.devices.reshape(4, 4, 4, 2), ("x", "y", "z", "c"))
    seq = ("x", "y")
    head = ("z", "c")
    placed = (
        P(seq, head),
        P(seq, None),
        P(seq, head, None),
        P(),
        P(seq, None),
        P(seq, None, None),
        P(head, None, None),
        P(head, None, None),
        P(head, None),
    )
    return jax.shard_map(
        per_device, mesh=fine, in_specs=placed, out_specs=P(seq, head), check_vma=False
    )
```

```python
import functools

import jax
import jax.numpy as jnp
from jax import lax
from jax.experimental import pallas as pl
from jax.experimental.pallas import tpu as pltpu
from jax.sharding import Mesh, PartitionSpec as P


MOST = 4
THETA = 50000.0
TILE = 128
NEG = -1e30
VMEM = pltpu.VMEM
SMEM = pltpu.SMEM


def vspec():
    return pl.BlockSpec(memory_space=VMEM)


def sspec():
    return pl.BlockSpec(memory_space=SMEM)


def params(mib):
    return pltpu.CompilerParams(vmem_limit_bytes=mib * 1024 * 1024)


def cost(flops, moved):
    return pl.CostEstimate(flops=int(flops), bytes_accessed=int(moved), transcendentals=0)


def dot_t(a, b):
    return lax.dot_general(a, b, (((1,), (1,)), ((), ())), preferred_element_type=jnp.float32)


def dot(a, b):
    return jnp.dot(a, b, preferred_element_type=jnp.float32)


def pick_kernel(slot_ref, list_ref, arrived_ref, cos_ref, sin_ref, out_ref):
    latent = out_ref.shape[2] - 64
    for j in range(out_ref.shape[0]):
        rows = arrived_ref[slot_ref[j]]
        out_ref[j, :, :latent] = rows[:, :latent]
        rotary = rows[:, latent:].astype(jnp.float32)
        swapped = jnp.concatenate([rotary[:, 32:], rotary[:, :32]], axis=1)
        turned = rotary * cos_ref[j][None, :] + swapped * sin_ref[j][None, :]
        out_ref[j, :, latent:] = turned.astype(jnp.bfloat16)


def pick(slots, lists, arrived, cosines, sines):
    count = slots.shape[0]
    return pl.pallas_call(
        pick_kernel,
        name="pick",
        out_shape=jax.ShapeDtypeStruct((count,) + arrived.shape[1:], jnp.bfloat16),
        in_specs=[sspec(), sspec(), vspec(), vspec(), vspec()],
        out_specs=vspec(),
        compiler_params=params(4),
        cost_estimate=cost(1e8, 2e6),
    )(slots, lists, arrived, cosines, sines)


def start_kernel(place_ref, mask_ref, q_ref, uk_ref, q_out, list_out):
    heads, nope, latent = uk_ref.shape
    rope = q_out.shape[2] - latent
    width = nope + rope
    tiles = q_ref.shape[0] // TILE
    listed = mask_ref.shape[1]
    room = list_out.shape[1] - 3
    for t in range(tiles):
        for j in range(room):
            list_out[t, j] = 0
        count = jnp.int32(0)
        for j in range(listed):
            list_out[t, count] = j
            count = count + (mask_ref[t, j] > 0).astype(jnp.int32)
        list_out[t, room] = count
        list_out[t, room + 1] = place_ref[0]
        list_out[t, room + 2] = place_ref[1]
    for h in range(heads):
        ql = dot(q_ref[:, h * width : h * width + nope], uk_ref[h]).astype(jnp.bfloat16)
        qr = q_ref[:, h * width + nope : (h + 1) * width]
        for t in range(tiles):
            q_out[t, h * TILE : (h + 1) * TILE, :latent] = ql[t * TILE : (t + 1) * TILE]
            q_out[t, h * TILE : (h + 1) * TILE, latent:] = qr[t * TILE : (t + 1) * TILE]


def start(place, tile_mask, queries, w_uk):
    tiles, listed = tile_mask.shape
    heads, nope, latent = w_uk.shape
    rope = queries.shape[1] // heads - nope
    return pl.pallas_call(
        start_kernel,
        name="start",
        out_shape=(
            jax.ShapeDtypeStruct((tiles, heads * TILE, latent + rope), jnp.bfloat16),
            jax.ShapeDtypeStruct((tiles, listed + 3), jnp.int32),
        ),
        in_specs=[sspec(), sspec(), vspec(), vspec()],
        out_specs=(vspec(), sspec()),
        compiler_params=params(16),
        cost_estimate=cost(4e9, 8e6),
    )(place, tile_mask, queries, w_uk)


def fold(s, v, t, scale, high_ref, sum_ref, acc_ref):
    old = high_ref[t]
    new = jnp.maximum(old, jnp.max(s, axis=1, keepdims=True))
    alpha = jnp.exp((old - new) * scale)
    width = s.shape[1] // 128
    p = jnp.exp((s - jnp.concatenate([new] * width, axis=1)) * scale)
    part = p[:, :128]
    for w in range(1, width):
        part = part + p[:, w * 128 : (w + 1) * 128]
    sum_ref[t] = sum_ref[t] * alpha + part
    high_ref[t] = new
    wide = jnp.concatenate([alpha] * (acc_ref.shape[2] // 128), axis=1)
    acc_ref[t] = acc_ref[t] * wide + dot(p.astype(jnp.bfloat16), v)


def attend(list_ref, q_ref, sources, group, scale, high_ref, sum_ref, acc_ref):
    latent = acc_ref.shape[2]
    tiles = q_ref.shape[0]
    per = len(sources) * sources[0].shape[1]
    room = list_ref.shape[1] - 3
    counts = [list_ref[t, room] for t in range(tiles)]
    most = functools.reduce(jnp.maximum, counts)

    def body(g, carry):
        keys, scores = [], []
        for t in range(tiles):
            rows = jnp.concatenate(
                [ref[list_ref[t, g * group + i]] for i in range(group) for ref in sources], axis=0
            )
            s = dot_t(q_ref[t], rows)
            col = lax.broadcasted_iota(jnp.int32, s.shape, 1)
            keys.append(rows)
            scores.append(jnp.where(col < (counts[t] - g * group) * per, s, NEG))
        for t in range(tiles):
            fold(scores[t], keys[t][:, :latent], t, scale, high_ref, sum_ref, acc_ref)
        return carry

    lax.fori_loop(0, (most + group - 1) // group, body, 0)


def first_kernel(
    list_ref, q_ref, own_ref, *refs, pieces, group, scale
):
    sources = refs[:pieces]
    high_ref, sum_ref, acc_ref = refs[pieces:]
    latent = acc_ref.shape[2]
    for t in range(q_ref.shape[0]):
        keys = own_ref[: (t + 1) * TILE]
        s = dot_t(q_ref[t], keys)
        row = lax.broadcasted_iota(jnp.int32, s.shape, 0) % TILE + t * TILE
        col = lax.broadcasted_iota(jnp.int32, s.shape, 1)
        s = jnp.where(col <= row, s, NEG)
        high = jnp.max(s, axis=1, keepdims=True)
        p = jnp.exp((s - high) * scale)
        part = p[:, :128]
        for w in range(1, t + 1):
            part = part + p[:, w * 128 : (w + 1) * 128]
        high_ref[t] = jnp.broadcast_to(high, high_ref.shape[1:])
        sum_ref[t] = part
        acc_ref[t] = dot(p.astype(jnp.bfloat16), keys[:, :latent])
    attend(list_ref, q_ref, sources, group, scale, high_ref, sum_ref, acc_ref)


def first(lists, q, own_rows, pieces, latent, group, scale):
    tiles, rows, _ = q.shape
    f32 = jnp.float32
    args = (lists, q, own_rows, *pieces)
    return pl.pallas_call(
        functools.partial(first_kernel, pieces=len(pieces), group=group, scale=scale),
        name="first",
        out_shape=(
            jax.ShapeDtypeStruct((tiles, rows, 128), f32),
            jax.ShapeDtypeStruct((tiles, rows, 128), f32),
            jax.ShapeDtypeStruct((tiles, rows, latent), f32),
        ),
        in_specs=[sspec()] + [vspec()] * (len(args) - 1),
        out_specs=(vspec(),) * 3,
        compiler_params=params(16),
        cost_estimate=cost(5e9, 2e7),
    )(*args)


def stage_kernel(list_ref, q_ref, *refs, pieces, group, scale):
    sources = refs[:pieces]
    high_in, sum_in, acc_in, high_ref, sum_ref, acc_ref = refs[pieces:]
    high_ref[...] = high_in[...]
    sum_ref[...] = sum_in[...]
    acc_ref[...] = acc_in[...]
    attend(list_ref, q_ref, sources, group, scale, high_ref, sum_ref, acc_ref)


def stage(lists, q, pieces, state, group, scale, flops):
    first = 2 + len(pieces)
    args = (lists, q, *pieces, *state)
    return pl.pallas_call(
        functools.partial(stage_kernel, pieces=len(pieces), group=group, scale=scale),
        name="stage",
        out_shape=tuple(jax.ShapeDtypeStruct(x.shape, x.dtype) for x in state),
        in_specs=[sspec()] + [vspec()] * (len(args) - 1),
        out_specs=(vspec(),) * 3,
        input_output_aliases={first: 0, first + 1: 1, first + 2: 2},
        compiler_params=params(16),
        cost_estimate=cost(flops, 2e7),
    )(*args)


def project(x, wo_ref, away, mine, list_ref, columns):
    room = list_ref.shape[1] - 3
    level, core = list_ref[0, room + 1], list_ref[0, room + 2]
    core = core if mine else 1 - core
    at = lax.rem(level + away, 4) * (2 * columns) + core * columns
    at = pl.multiple_of(at, 128)
    return dot(x, wo_ref[:, pl.ds(at, columns)]).astype(jnp.bfloat16)


def last_kernel(list_ref, q_ref, *refs, pieces, group, scale):
    halves = refs[:pieces]
    uv_ref, wo_ref, high_in, sum_in, acc_in = refs[pieces : pieces + 5]
    out_ref, mine_ref, other_ref, high_ref, sum_ref, acc_ref, near = refs[pieces + 5 :]
    high_ref[...] = high_in[...]
    sum_ref[...] = sum_in[...]
    acc_ref[...] = acc_in[...]
    spans = halves[0].shape[0]
    for i in range(pieces):
        near[i // 2, (i % 2) * spans : (i % 2 + 1) * spans] = halves[i][...]
    sources = [near.at[i] for i in range(pieces // 2)]
    attend(list_ref, q_ref, sources, group, scale, high_ref, sum_ref, acc_ref)
    for t in range(q_ref.shape[0]):
        total = jnp.sum(sum_ref[t], axis=1, keepdims=True)
        mixed = (acc_ref[t] / total).astype(jnp.bfloat16)
        for h in range(uv_ref.shape[0]):
            out_ref[t * TILE : (t + 1) * TILE, h * 128 : (h + 1) * 128] = dot(
                mixed[h * TILE : (h + 1) * TILE], uv_ref[h]
            ).astype(jnp.bfloat16)
    columns = mine_ref.shape[1]
    x = out_ref[...]
    other_ref[...] = project(x, wo_ref, 2, False, list_ref, columns)
    mine_ref[...] = project(x, wo_ref, 2, True, list_ref, columns)


def last(lists, q, halves, w_uv, state, w_o, group, scale):
    tiles, _, _ = state[2].shape
    tokens = tiles * TILE
    columns = w_o.shape[1] // 8
    bf = jnp.bfloat16
    args = (lists, q, *halves, w_uv, w_o, *state)
    first = len(args) - 3
    shape = halves[0].shape
    outs = pl.pallas_call(
        functools.partial(last_kernel, pieces=len(halves), group=group, scale=scale),
        name="last",
        out_shape=(
            jax.ShapeDtypeStruct((tokens, w_o.shape[0]), bf),
            jax.ShapeDtypeStruct((tokens, columns), bf),
            jax.ShapeDtypeStruct((tokens, columns), bf),
        )
        + tuple(jax.ShapeDtypeStruct(x.shape, x.dtype) for x in state),
        in_specs=[sspec()] + [vspec()] * (len(args) - 1),
        out_specs=(vspec(),) * 6,
        input_output_aliases={first: 3, first + 1: 4, first + 2: 5},
        scratch_shapes=[pltpu.VMEM((len(halves) // 2, 2 * shape[0]) + shape[1:], bf)],
        compiler_params=params(16),
        cost_estimate=cost(8e9, 2e7),
    )(*args)
    return outs[:3]


def rest_kernel(list_ref, x_ref, wo_ref, other_ref, mine_ref):
    columns = other_ref.shape[2]
    x = x_ref[...]
    for i, away in enumerate((1, 3, 0)):
        other_ref[i] = project(x, wo_ref, away, False, list_ref, columns)
    for i, away in enumerate((1, 3, 0)):
        mine_ref[i] = project(x, wo_ref, away, True, list_ref, columns)


def rest(lists, head_out, w_o):
    shape = jax.ShapeDtypeStruct((3, head_out.shape[0], w_o.shape[1] // 8), jnp.bfloat16)
    return pl.pallas_call(
        rest_kernel,
        name="rest",
        out_shape=(shape, shape),
        in_specs=[sspec(), vspec(), vspec()],
        out_specs=(vspec(), vspec()),
        compiler_params=params(8),
        cost_estimate=cost(3e9, 1.2e7),
    )(lists, head_out, w_o)


def per_device(queries, own_latent, cache, block_list, offsets, tile_mask, w_uk, w_uv, w_o):
    seq = ("x", "y")
    seq_count = lax.axis_size(seq)
    seq_index = lax.axis_index(seq)
    spans_held = cache.shape[0]
    latent_full = cache.shape[2]
    listed_count = block_list.shape[1]
    latent = w_uk.shape[2]
    rope = latent_full - latent
    width = w_uk.shape[1] + rope
    scale = width ** (-0.5)

    owners = block_list // spans_held
    within = block_list % spans_held
    earlier = jnp.tril(jnp.ones((listed_count, listed_count), jnp.bool_), -1)
    same_owner = owners[:, :, None] == owners[:, None, :]
    ranking = jnp.sum(same_owner & earlier[None], axis=2)
    slot_ids = jnp.arange(MOST, dtype=jnp.int32)
    matches = (owners == seq_index)[:, :, None] & (ranking[:, :, None] == slot_ids[None, None, :])
    send_index = jnp.sum(jnp.where(matches, within[:, :, None], 0), axis=1)
    my_owners = lax.dynamic_index_in_dim(owners, seq_index, 0, keepdims=False)
    my_ranking = lax.dynamic_index_in_dim(ranking, seq_index, 0, keepdims=False)
    flat_slot = my_owners * MOST + my_ranking
    sent = cache[send_index]
    arrived = lax.all_to_all(sent, seq, split_axis=0, concat_axis=0, tiled=True)

    place = jnp.stack([lax.axis_index("z"), lax.axis_index("c")]).astype(jnp.int32)
    inverse = THETA ** (-jnp.arange(rope // 2, dtype=jnp.float32) * 2.0 / rope)
    angles = offsets[0].astype(jnp.float32)[:, None] * inverse[None, :]
    cosine = jnp.cos(angles)
    sine = jnp.sin(angles)
    cosines = jnp.concatenate([cosine, cosine], axis=1)
    sines = jnp.concatenate([-sine, sine], axis=1)
    q, lists = start(place, tile_mask[0], queries, w_uk)

    own = pick(
        flat_slot,
        lists,
        arrived.reshape(seq_count * MOST, cache.shape[1], latent_full),
        cosines,
        sines,
    )
    size = 4
    up = [(i, (i + 1) % size) for i in range(size)]
    down = [(i, (i - 1) % size) for i in range(size)]
    swap = [(0, 1), (1, 0)]

    def other_core(x):
        return lax.ppermute(x, "c", swap)

    half = own.shape[0] // 2
    plus = lax.ppermute(own, "z", up)
    minus = lax.ppermute(own, "z", down)
    twin = other_core(own)
    state = first(lists, q, own_latent, [own, twin], latent, 16, scale)
    far_low = lax.ppermute(plus[:half], "z", up)
    far_high = lax.ppermute(minus[half:], "z", down)
    pieces = [plus, minus]
    pieces = pieces + [other_core(x) for x in pieces]
    state = stage(lists, q, pieces, state, 8, scale, 1e10)
    halves = [far_low, far_high]
    halves = halves + [other_core(x) for x in halves]
    head_out, far_mine, far_other = last(
        lists, q, halves, w_uv, state, w_o, 16, scale
    )

    bf = jnp.bfloat16
    f32 = jnp.float32

    def add(*terms):
        return functools.reduce(jnp.add, [x.astype(f32) for x in terms])

    h = far_mine.shape[0] // 2
    far = add(far_mine, other_core(far_other)).astype(bf)
    from_below = lax.ppermute(far[:h], "z", up)
    from_above = lax.ppermute(far[h:], "z", down)
    others, mine = rest(lists, head_out, w_o)
    others = other_core(others)
    early_up = lax.ppermute(add(mine[0, h:], others[0, h:]).astype(bf), "z", up)
    early_down = lax.ppermute(add(mine[1, :h], others[1, :h]).astype(bf), "z", down)
    late_up = lax.ppermute(add(mine[0, :h], others[0, :h], from_below).astype(bf), "z", up)
    late_down = lax.ppermute(add(mine[1, h:], others[1, h:], from_above).astype(bf), "z", down)
    kept = add(mine[2], others[2])
    top = add(kept[:h], late_up, early_down)
    bottom = add(kept[h:], early_up, late_down)
    return jnp.concatenate([top, bottom], axis=0).astype(bf)


def solution(mesh):
    fine = Mesh(mesh.devices.reshape(4, 4, 4, 2), ("x", "y", "z", "c"))
    seq = ("x", "y")
    head = ("z", "c")
    placed = (
        P(seq, head),
        P(seq, None),
        P(seq, head, None),
        P(),
        P(seq, None),
        P(seq, None, None),
        P(head, None, None),
        P(head, None, None),
        P(head, None),
    )
    return jax.shard_map(
        per_device, mesh=fine, in_specs=placed, out_specs=P(seq, head), check_vma=False
    )
```

```python
import functools

import jax
import jax.numpy as jnp
from jax import lax
from jax.experimental import pallas as pl
from jax.experimental.pallas import tpu as pltpu
from jax.sharding import Mesh, PartitionSpec as P


MOST = 4
THETA = 50000.0
TILE = 128
NEG = -1e30
VMEM = pltpu.VMEM
SMEM = pltpu.SMEM


def vspec():
    return pl.BlockSpec(memory_space=VMEM)


def sspec():
    return pl.BlockSpec(memory_space=SMEM)


def params(mib):
    return pltpu.CompilerParams(vmem_limit_bytes=mib * 1024 * 1024)


def cost(flops, moved):
    return pl.CostEstimate(flops=int(flops), bytes_accessed=int(moved), transcendentals=0)


def dot_t(a, b):
    return lax.dot_general(a, b, (((1,), (1,)), ((), ())), preferred_element_type=jnp.float32)


def dot(a, b):
    return jnp.dot(a, b, preferred_element_type=jnp.float32)


def pick_kernel(slot_ref, list_ref, arrived_ref, cos_ref, sin_ref, out_ref):
    latent = out_ref.shape[2] - 64
    for j in range(out_ref.shape[0]):
        rows = arrived_ref[slot_ref[j]]
        out_ref[j, :, :latent] = rows[:, :latent]
        rotary = rows[:, latent:].astype(jnp.float32)
        swapped = jnp.concatenate([rotary[:, 32:], rotary[:, :32]], axis=1)
        turned = rotary * cos_ref[j][None, :] + swapped * sin_ref[j][None, :]
        out_ref[j, :, latent:] = turned.astype(jnp.bfloat16)


def pick(slots, lists, arrived, cosines, sines):
    count = slots.shape[0]
    return pl.pallas_call(
        pick_kernel,
        name="pick",
        out_shape=jax.ShapeDtypeStruct((count,) + arrived.shape[1:], jnp.bfloat16),
        in_specs=[sspec(), sspec(), vspec(), vspec(), vspec()],
        out_specs=vspec(),
        compiler_params=params(4),
        cost_estimate=cost(1e8, 2e6),
    )(slots, lists, arrived, cosines, sines)


def start_kernel(place_ref, mask_ref, q_ref, uk_ref, q_out, list_out):
    heads, nope, latent = uk_ref.shape
    rope = q_out.shape[2] - latent
    width = nope + rope
    tiles = q_ref.shape[0] // TILE
    listed = mask_ref.shape[1]
    room = list_out.shape[1] - 3
    for t in range(tiles):
        for j in range(room):
            list_out[t, j] = 0
        count = jnp.int32(0)
        for j in range(listed):
            list_out[t, count] = j
            count = count + (mask_ref[t, j] > 0).astype(jnp.int32)
        list_out[t, room] = count
        list_out[t, room + 1] = place_ref[0]
        list_out[t, room + 2] = place_ref[1]
    for h in range(heads):
        ql = dot(q_ref[:, h * width : h * width + nope], uk_ref[h]).astype(jnp.bfloat16)
        qr = q_ref[:, h * width + nope : (h + 1) * width]
        for t in range(tiles):
            q_out[t, h * TILE : (h + 1) * TILE, :latent] = ql[t * TILE : (t + 1) * TILE]
            q_out[t, h * TILE : (h + 1) * TILE, latent:] = qr[t * TILE : (t + 1) * TILE]


def start(place, tile_mask, queries, w_uk):
    tiles, listed = tile_mask.shape
    heads, nope, latent = w_uk.shape
    rope = queries.shape[1] // heads - nope
    return pl.pallas_call(
        start_kernel,
        name="start",
        out_shape=(
            jax.ShapeDtypeStruct((tiles, heads * TILE, latent + rope), jnp.bfloat16),
            jax.ShapeDtypeStruct((tiles, listed + 3), jnp.int32),
        ),
        in_specs=[sspec(), sspec(), vspec(), vspec()],
        out_specs=(vspec(), sspec()),
        compiler_params=params(16),
        cost_estimate=cost(4e9, 8e6),
    )(place, tile_mask, queries, w_uk)


def fold(s, v, t, scale, state):
    high_ref, sum_ref, acc_ref = state
    old = high_ref[t]
    new = jnp.maximum(old, jnp.max(s, axis=1, keepdims=True))
    alpha = jnp.exp((old - new) * scale)
    width = s.shape[1] // 128
    p = jnp.exp((s - jnp.concatenate([new] * width, axis=1)) * scale)
    part = p[:, :128]
    for w in range(1, width):
        part = part + p[:, w * 128 : (w + 1) * 128]
    sum_ref[t] = sum_ref[t] * alpha + part
    high_ref[t] = new
    wide = jnp.concatenate([alpha] * (acc_ref.shape[2] // 128), axis=1)
    acc_ref[t] = acc_ref[t] * wide + dot(p.astype(jnp.bfloat16), v)


def gather(halves, near):
    spans = halves[0].shape[0]
    for i, half in enumerate(halves):
        near[i // 2, (i % 2) * spans : (i % 2 + 1) * spans] = half[...]


def attend(list_ref, q_ref, sources, scale, state, short):
    latent = state[2].shape[2]
    tiles = q_ref.shape[0]
    per = len(sources) * sources[0].shape[1]
    group = 512 // per
    room = list_ref.shape[1] - 3
    counts = [list_ref[t, room] for t in range(tiles)]

    def step(base, size, which):
        keys, scores = [], []
        for t in which:
            rows = jnp.concatenate(
                [ref[list_ref[t, base + i]] for i in range(size) for ref in sources], axis=0
            )
            s = dot_t(q_ref[t], rows)
            col = lax.broadcasted_iota(jnp.int32, s.shape, 1)
            keys.append(rows)
            scores.append(jnp.where(col < (list_ref[t, room] - base) * per, s, NEG))
        for i, t in enumerate(which):
            fold(scores[i], keys[i][:, :latent], t, scale, state)

    low, high = jnp.minimum(counts[0], counts[1]), jnp.maximum(counts[0], counts[1])
    longer = (counts[1] > counts[0]).astype(jnp.int32)
    full = low // group
    left = low - full * group
    wide = left > group // 2 if short else left > 0
    steps = full + wide.astype(jnp.int32)
    done = steps * group

    def body(g, carry):
        step(g * group, group, range(tiles))
        return carry

    lax.fori_loop(0, steps, body, 0)
    if short:
        narrow = jnp.logical_and(left > 0, left <= group // 2)
        done = done + jnp.where(narrow, group // 2, 0)

        @pl.when(narrow)
        def _():
            step(full * group, group // 2, range(tiles))

    def rest_of_longer(g, carry):
        step(done + g * group, group, (longer,))
        return carry

    lax.fori_loop(0, (jnp.maximum(high - done, 0) + group - 1) // group, rest_of_longer, 0)


def first_kernel(list_ref, q_ref, own_ref, *refs, pieces, scale):
    sources, state = refs[:pieces], refs[pieces:]
    high_ref, sum_ref, acc_ref = state
    latent = acc_ref.shape[2]
    for t in range(q_ref.shape[0]):
        keys = own_ref[: (t + 1) * TILE]
        s = dot_t(q_ref[t], keys)
        row = lax.broadcasted_iota(jnp.int32, s.shape, 0) % TILE + t * TILE
        col = lax.broadcasted_iota(jnp.int32, s.shape, 1)
        s = jnp.where(col <= row, s, NEG)
        high = jnp.max(s, axis=1, keepdims=True)
        p = jnp.exp((s - high) * scale)
        part = p[:, :128]
        for w in range(1, t + 1):
            part = part + p[:, w * 128 : (w + 1) * 128]
        high_ref[t] = jnp.broadcast_to(high, high_ref.shape[1:])
        sum_ref[t] = part
        acc_ref[t] = dot(p.astype(jnp.bfloat16), keys[:, :latent])
    attend(list_ref, q_ref, sources, scale, state, False)


def near_scratch(halves):
    shape = halves[0].shape
    return pltpu.VMEM((len(halves) // 2, 2 * shape[0]) + shape[1:], halves[0].dtype)


def first(lists, q, own_rows, halves, latent, scale):
    tiles, rows, _ = q.shape
    f32 = jnp.float32
    args = (lists, q, own_rows, *halves)
    return pl.pallas_call(
        functools.partial(first_kernel, pieces=len(halves), scale=scale),
        name="first",
        out_shape=(
            jax.ShapeDtypeStruct((tiles, rows, 128), f32),
            jax.ShapeDtypeStruct((tiles, rows, 128), f32),
            jax.ShapeDtypeStruct((tiles, rows, latent), f32),
        ),
        in_specs=[sspec()] + [vspec()] * (len(args) - 1),
        out_specs=(vspec(),) * 3,
        compiler_params=params(16),
        cost_estimate=cost(5e9, 2e7),
    )(*args)


def stage_kernel(list_ref, q_ref, *refs, pieces, scale):
    sources = refs[:pieces]
    source, state = refs[pieces : pieces + 3], refs[pieces + 3 : pieces + 6]
    for old, new in zip(source, state):
        new[...] = old[...]
    attend(list_ref, q_ref, sources, scale, state, True)


def stage(lists, q, halves, state, scale):
    before = 2 + len(halves)
    args = (lists, q, *halves, *state)
    return pl.pallas_call(
        functools.partial(stage_kernel, pieces=len(halves), scale=scale),
        name="stage",
        out_shape=tuple(jax.ShapeDtypeStruct(x.shape, x.dtype) for x in state),
        in_specs=[sspec()] + [vspec()] * (len(args) - 1),
        out_specs=(vspec(),) * 3,
        input_output_aliases={before: 0, before + 1: 1, before + 2: 2},
        compiler_params=params(18),
        cost_estimate=cost(1e10, 2e7),
    )(*args)


def project(x, wo_ref, away, mine, list_ref, columns):
    room = list_ref.shape[1] - 3
    level, core = list_ref[0, room + 1], list_ref[0, room + 2]
    core = core if mine else 1 - core
    at = lax.rem(level + away, 4) * (2 * columns) + core * columns
    at = pl.multiple_of(at, 128)
    return dot(x, wo_ref[:, pl.ds(at, columns)]).astype(jnp.bfloat16)


def last_kernel(list_ref, q_ref, *refs, pieces, scale):
    halves = refs[:pieces]
    uv_ref, wo_ref = refs[pieces : pieces + 2]
    source = refs[pieces + 2 : pieces + 5]
    out_ref, mine_ref, other_ref = refs[pieces + 5 : pieces + 8]
    state, near = refs[pieces + 8 : pieces + 11], refs[pieces + 11]
    gather(halves, near)
    for old, new in zip(source, state):
        new[...] = old[...]
    sources = [near.at[i] for i in range(near.shape[0])]
    attend(list_ref, q_ref, sources, scale, state, True)
    for t in range(q_ref.shape[0]):
        total = jnp.sum(state[1][t], axis=1, keepdims=True)
        mixed = (state[2][t] / total).astype(jnp.bfloat16)
        for h in range(uv_ref.shape[0]):
            out_ref[t * TILE : (t + 1) * TILE, h * 128 : (h + 1) * 128] = dot(
                mixed[h * TILE : (h + 1) * TILE], uv_ref[h]
            ).astype(jnp.bfloat16)
    columns = mine_ref.shape[1]
    x = out_ref[...]
    other_ref[...] = project(x, wo_ref, 2, False, list_ref, columns)
    mine_ref[...] = project(x, wo_ref, 2, True, list_ref, columns)


def last(lists, q, halves, w_uv, state, w_o, scale):
    tiles, _, _ = state[2].shape
    tokens = tiles * TILE
    columns = w_o.shape[1] // 8
    bf = jnp.bfloat16
    args = (lists, q, *halves, w_uv, w_o, *state)
    before = len(args) - 3
    outs = pl.pallas_call(
        functools.partial(last_kernel, pieces=len(halves), scale=scale),
        name="last",
        out_shape=(
            jax.ShapeDtypeStruct((tokens, w_o.shape[0]), bf),
            jax.ShapeDtypeStruct((tokens, columns), bf),
            jax.ShapeDtypeStruct((tokens, columns), bf),
        )
        + tuple(jax.ShapeDtypeStruct(x.shape, x.dtype) for x in state),
        in_specs=[sspec()] + [vspec()] * (len(args) - 1),
        out_specs=(vspec(),) * 6,
        input_output_aliases={before: 3, before + 1: 4, before + 2: 5},
        scratch_shapes=[near_scratch(halves)],
        compiler_params=params(16),
        cost_estimate=cost(8e9, 2e7),
    )(*args)
    return outs[:3]


def columns_kernel(list_ref, x_ref, wo_ref, other_ref, mine_ref, *, aways):
    columns = other_ref.shape[2]
    x = x_ref[...]
    for i, away in enumerate(aways):
        other_ref[i] = project(x, wo_ref, away, False, list_ref, columns)
    for i, away in enumerate(aways):
        mine_ref[i] = project(x, wo_ref, away, True, list_ref, columns)


def columns_of(lists, head_out, w_o, aways):
    tokens = head_out.shape[0]
    shape = jax.ShapeDtypeStruct((len(aways), tokens, w_o.shape[1] // 8), jnp.bfloat16)
    return pl.pallas_call(
        functools.partial(columns_kernel, aways=aways),
        name="columns",
        out_shape=(shape, shape),
        in_specs=[sspec(), vspec(), vspec()],
        out_specs=(vspec(), vspec()),
        compiler_params=params(8),
        cost_estimate=cost(1e9 * len(aways), 4e6 * len(aways)),
    )(lists, head_out, w_o)


def finish_kernel(mine_ref, other_ref, *refs):
    out_ref = refs[-1]
    half = refs[0].shape[0]
    f32 = jnp.float32
    for i in range(2):
        rows = pl.ds(i * half, half)
        total = mine_ref[0, rows].astype(f32) + other_ref[0, rows].astype(f32)
        for ref in refs[2 * i : 2 * i + 2]:
            total = total + ref[...].astype(f32)
        out_ref[rows] = total.astype(jnp.bfloat16)


def finish(mine, other, top, bottom):
    args = (mine, other, *top, *bottom)
    return pl.pallas_call(
        finish_kernel,
        name="finish",
        out_shape=jax.ShapeDtypeStruct(mine.shape[1:], jnp.bfloat16),
        in_specs=[vspec()] * len(args),
        out_specs=vspec(),
        compiler_params=params(8),
    )(*args)


def per_device(queries, own_latent, cache, block_list, offsets, tile_mask, w_uk, w_uv, w_o):
    seq = ("x", "y")
    seq_count = lax.axis_size(seq)
    seq_index = lax.axis_index(seq)
    spans_held = cache.shape[0]
    listed_count = block_list.shape[1]
    latent_full = cache.shape[2]
    latent = w_uk.shape[2]
    rope = latent_full - latent
    width = w_uk.shape[1] + rope
    scale = width ** (-0.5)

    owners = block_list // spans_held
    within = block_list % spans_held
    earlier = jnp.tril(jnp.ones((listed_count, listed_count), jnp.bool_), -1)
    same_owner = owners[:, :, None] == owners[:, None, :]
    ranking = jnp.sum(same_owner & earlier[None], axis=2)
    slot_ids = jnp.arange(MOST, dtype=jnp.int32)
    matches = (owners == seq_index)[:, :, None] & (ranking[:, :, None] == slot_ids[None, None, :])
    send_index = jnp.sum(jnp.where(matches, within[:, :, None], 0), axis=1)
    my_owners = lax.dynamic_index_in_dim(owners, seq_index, 0, keepdims=False)
    my_ranking = lax.dynamic_index_in_dim(ranking, seq_index, 0, keepdims=False)
    flat_slot = my_owners * MOST + my_ranking
    sent = cache[send_index]
    arrived = lax.all_to_all(sent, seq, split_axis=0, concat_axis=0, tiled=True)

    place = jnp.stack([lax.axis_index("z"), lax.axis_index("c")]).astype(jnp.int32)
    inverse = THETA ** (-jnp.arange(rope // 2, dtype=jnp.float32) * 2.0 / rope)
    angles = offsets[0].astype(jnp.float32)[:, None] * inverse[None, :]
    cosine = jnp.cos(angles)
    sine = jnp.sin(angles)
    cosines = jnp.concatenate([cosine, cosine], axis=1)
    sines = jnp.concatenate([-sine, sine], axis=1)
    q, lists = start(place, tile_mask[0], queries, w_uk)

    own = pick(
        flat_slot,
        lists,
        arrived.reshape(seq_count * MOST, cache.shape[1], latent_full),
        cosines,
        sines,
    )
    size = 4
    up = [(i, (i + 1) % size) for i in range(size)]
    down = [(i, (i - 1) % size) for i in range(size)]
    swap = [(0, 1), (1, 0)]

    def other_core(x):
        return lax.ppermute(x, "c", swap)

    def move(x, ways):
        return lax.ppermute(x, "z", ways)

    plus = move(own, up)
    minus = move(own, down)
    twin = other_core(own)
    state = first(lists, q, own_latent, [own, twin], latent, scale)
    half = own.shape[0] // 2
    low = move(plus[:half], up)
    high = move(minus[half:], down)
    pieces = [plus, minus]
    pieces = pieces + [other_core(x) for x in pieces]
    state = stage(lists, q, pieces, state, scale)
    halves = [low, high]
    halves = halves + [other_core(x) for x in halves]
    head_out, far_mine, far_other = last(lists, q, halves, w_uv, state, w_o, scale)

    bf = jnp.bfloat16
    f32 = jnp.float32

    def add(*terms):
        return functools.reduce(jnp.add, [x.astype(f32) for x in terms])

    h = far_mine.shape[0] // 2
    far_other = other_core(far_other)
    others, mine = columns_of(lists, head_out, w_o, (1, 3))
    others = other_core(others)
    far = add(far_mine, far_other).astype(bf)
    below = move(far[:h], up)
    above = move(far[h:], down)
    early_up = move(add(mine[0, h:], others[0, h:]).astype(bf), up)
    early_down = move(add(mine[1, :h], others[1, :h]).astype(bf), down)
    kept_other, kept_mine = columns_of(lists, head_out, w_o, (0,))
    late_up = move(add(mine[0, :h], others[0, :h], below).astype(bf), up)
    late_down = move(add(mine[1, h:], others[1, h:], above).astype(bf), down)
    kept_other = other_core(kept_other)
    return finish(kept_mine, kept_other, (late_up, early_down), (early_up, late_down))


def solution(mesh):
    fine = Mesh(mesh.devices.reshape(4, 4, 4, 2), ("x", "y", "z", "c"))
    seq = ("x", "y")
    head = ("z", "c")
    placed = (
        P(seq, head),
        P(seq, None),
        P(seq, head, None),
        P(),
        P(seq, None),
        P(seq, None, None),
        P(head, None, None),
        P(head, None, None),
        P(head, None),
    )
    return jax.shard_map(
        per_device, mesh=fine, in_specs=placed, out_specs=P(seq, head), check_vma=False
    )
```

```python
import functools

import jax
import jax.numpy as jnp
from jax import lax
from jax.experimental import pallas as pl
from jax.experimental.pallas import tpu as pltpu
from jax.sharding import Mesh, PartitionSpec as P


MOST = 4
THETA = 50000.0
TILE = 128
NEG = -1e30
VMEM = pltpu.VMEM
SMEM = pltpu.SMEM


def vspec():
    return pl.BlockSpec(memory_space=VMEM)


def sspec():
    return pl.BlockSpec(memory_space=SMEM)


def params(mib):
    return pltpu.CompilerParams(vmem_limit_bytes=mib * 1024 * 1024)


def cost(flops, moved):
    return pl.CostEstimate(flops=int(flops), bytes_accessed=int(moved), transcendentals=0)


def dot_t(a, b):
    return lax.dot_general(a, b, (((1,), (1,)), ((), ())), preferred_element_type=jnp.float32)


def dot(a, b):
    return jnp.dot(a, b, preferred_element_type=jnp.float32)


def send_kernel(index_ref, cache_ref, out_ref):
    readers = out_ref.shape[0]
    for r in range(readers):
        for k in range(0, MOST, 2):
            rotary = []
            for i in range(2):
                rows = cache_ref[index_ref[r, k + i]]
                for b in range(4):
                    out_ref[r, 4 * (k + i) + b] = rows[:, 128 * b : 128 * (b + 1)]
                rotary.append(rows[:, 512:])
            out_ref[r, 4 * MOST + k // 2] = jnp.concatenate(rotary, axis=1)


def send(index, cache):
    rows = cache.shape[1]
    shape = (index.shape[0], 4 * MOST + MOST // 2, rows, 128)
    return pl.pallas_call(
        send_kernel,
        name="send",
        out_shape=jax.ShapeDtypeStruct(shape, cache.dtype),
        in_specs=[sspec(), vspec()],
        out_specs=vspec(),
        compiler_params=params(4),
    )(index, cache)


def pick_kernel(slot_ref, list_ref, arrived_ref, cos_ref, sin_ref, out_ref):
    half = out_ref.shape[1] * 2 // 9
    for j in range(0, 2 * half, 2):
        h, i = j // half, j % half
        pair = []
        for e in range(2):
            owner = slot_ref[j + e] >> 2
            slot = slot_ref[j + e] & (MOST - 1)
            for b in range(4):
                out_ref[h, 4 * (i + e) + b] = arrived_ref[owner, 4 * slot + b]
            both = arrived_ref[owner, 4 * MOST + (slot >> 1)].astype(jnp.float32)
            rotary = jnp.where((slot & 1) == 1, both[:, 64:], both[:, :64])
            swapped = jnp.concatenate([rotary[:, 32:], rotary[:, :32]], axis=1)
            turned = rotary * cos_ref[j + e][None, :] + swapped * sin_ref[j + e][None, :]
            pair.append(turned)
        out_ref[h, 4 * half + i // 2] = jnp.concatenate(pair, axis=1).astype(jnp.bfloat16)


def pick(slots, lists, arrived, cosines, sines):
    half = slots.shape[0] // 2
    shape = (2, 4 * half + half // 2) + arrived.shape[2:]
    return pl.pallas_call(
        pick_kernel,
        name="pick",
        out_shape=jax.ShapeDtypeStruct(shape, jnp.bfloat16),
        in_specs=[sspec(), sspec(), vspec(), vspec(), vspec()],
        out_specs=vspec(),
        compiler_params=params(4),
        cost_estimate=cost(1e8, 2e6),
    )(slots, lists, arrived, cosines, sines)


def start_kernel(place_ref, mask_ref, q_ref, uk_ref, q_out, list_out):
    heads, nope, latent = uk_ref.shape
    rope = (q_out.shape[2] - latent) // 2
    width = nope + rope
    tiles = q_ref.shape[0] // TILE
    listed = mask_ref.shape[1]
    room = list_out.shape[1] - 3
    for t in range(tiles):
        for j in range(room):
            list_out[t, j] = 0
        count = jnp.int32(0)
        for j in range(listed):
            list_out[t, count] = j
            count = count + (mask_ref[t, j] > 0).astype(jnp.int32)
        list_out[t, room] = count
        list_out[t, room + 1] = place_ref[0]
        list_out[t, room + 2] = place_ref[1]
    for h in range(heads):
        ql = dot(q_ref[:, h * width : h * width + nope], uk_ref[h]).astype(jnp.bfloat16)
        qr = q_ref[:, h * width + nope : (h + 1) * width]
        for t in range(tiles):
            q_out[t, h * TILE : (h + 1) * TILE, :latent] = ql[t * TILE : (t + 1) * TILE]
            twice = jnp.concatenate([qr[t * TILE : (t + 1) * TILE]] * 2, axis=1)
            q_out[t, h * TILE : (h + 1) * TILE, latent:] = twice


def start(place, tile_mask, queries, w_uk):
    tiles, listed = tile_mask.shape
    heads, nope, latent = w_uk.shape
    rope = queries.shape[1] // heads - nope
    return pl.pallas_call(
        start_kernel,
        name="start",
        out_shape=(
            jax.ShapeDtypeStruct((tiles, heads * TILE, latent + 2 * rope), jnp.bfloat16),
            jax.ShapeDtypeStruct((tiles, listed + 3), jnp.int32),
        ),
        in_specs=[sspec(), sspec(), vspec(), vspec()],
        out_specs=(vspec(), sspec()),
        compiler_params=params(16),
        cost_estimate=cost(4e9, 8e6),
    )(place, tile_mask, queries, w_uk)


def fold(s, v, t, scale, state):
    high_ref, sum_ref, acc_ref = state
    old = high_ref[t]
    new = jnp.maximum(old, jnp.max(s, axis=1, keepdims=True))
    alpha = jnp.exp((old - new) * scale)
    width = s.shape[1] // 128
    p = jnp.exp((s - jnp.concatenate([new] * width, axis=1)) * scale)
    part = p[:, :128]
    for w in range(1, width):
        part = part + p[:, w * 128 : (w + 1) * 128]
    sum_ref[t] = sum_ref[t] * alpha + part
    high_ref[t] = new
    wide = jnp.concatenate([alpha] * (acc_ref.shape[2] // 128), axis=1)
    acc_ref[t] = acc_ref[t] * wide + dot(p.astype(jnp.bfloat16), v)


def gather(halves, near):
    for i, half in enumerate(halves):
        near[i // 2, i % 2] = half[...]


def sides(side_ref):
    lane = lax.broadcasted_iota(jnp.int32, side_ref.shape[1:], 1)
    for e in range(2):
        side_ref[e] = jnp.where((lane >= 64) == (e == 1), 1.0, 0.0).astype(jnp.bfloat16)


def span_rows(ref, j, side_ref):
    half = ref.shape[1] * 2 // 9
    h = (j >= half).astype(jnp.int32)
    i = j - h * half
    parts = [ref[h, 4 * i + b] for b in range(4)]
    parts.append(ref[h, 4 * half + (i >> 1)] * side_ref[i & 1])
    return jnp.concatenate(parts, axis=1)


def attend(list_ref, q_ref, sources, scale, state, side_ref, short):
    latent = state[2].shape[2]
    tiles = q_ref.shape[0]
    sides(side_ref)
    per = len(sources) * sources[0].shape[2]
    group = 512 // per
    room = list_ref.shape[1] - 3
    counts = [list_ref[t, room] for t in range(tiles)]

    def step(base, size, which):
        keys, scores = [], []
        for t in which:
            spans = [list_ref[t, base + i] for i in range(size)]
            rows = jnp.concatenate(
                [span_rows(ref, j, side_ref) for j in spans for ref in sources], axis=0
            )
            s = dot_t(q_ref[t], rows)
            col = lax.broadcasted_iota(jnp.int32, s.shape, 1)
            keys.append(rows)
            scores.append(jnp.where(col < (list_ref[t, room] - base) * per, s, NEG))
        for i, t in enumerate(which):
            fold(scores[i], keys[i][:, :latent], t, scale, state)

    low, high = jnp.minimum(counts[0], counts[1]), jnp.maximum(counts[0], counts[1])
    if not short:
        low = high
    full = low // group
    left = low - full * group
    wide = left > group // 2 if short else left > 0
    steps = full + wide.astype(jnp.int32)

    def body(g, carry):
        step(g * group, group, range(tiles))
        return carry

    lax.fori_loop(0, steps, body, 0)
    if not short:
        return
    narrow = jnp.logical_and(left > 0, left <= group // 2)
    done = steps * group + jnp.where(narrow, group // 2, 0)

    @pl.when(narrow)
    def _():
        step(full * group, group // 2, range(tiles))

    longer = (counts[1] > counts[0]).astype(jnp.int32)

    def rest_of_longer(g, carry):
        step(done + g * group, group, (longer,))
        return carry

    lax.fori_loop(0, (jnp.maximum(high - done, 0) + group - 1) // group, rest_of_longer, 0)


def first_kernel(list_ref, q_ref, own_ref, *refs, pieces, scale):
    sources, state, side_ref = refs[:pieces], refs[pieces:-1], refs[-1]
    high_ref, sum_ref, acc_ref = state
    latent = acc_ref.shape[2]
    for t in range(q_ref.shape[0]):
        keys = own_ref[: (t + 1) * TILE]
        s = dot_t(q_ref[t, :, : keys.shape[1]], keys)
        row = lax.broadcasted_iota(jnp.int32, s.shape, 0) % TILE + t * TILE
        col = lax.broadcasted_iota(jnp.int32, s.shape, 1)
        s = jnp.where(col <= row, s, NEG)
        high = jnp.max(s, axis=1, keepdims=True)
        p = jnp.exp((s - high) * scale)
        part = p[:, :128]
        for w in range(1, t + 1):
            part = part + p[:, w * 128 : (w + 1) * 128]
        high_ref[t] = jnp.broadcast_to(high, high_ref.shape[1:])
        sum_ref[t] = part
        acc_ref[t] = dot(p.astype(jnp.bfloat16), keys[:, :latent])
    attend(list_ref, q_ref, sources, scale, state, side_ref, False)


def near_scratch(halves):
    return pltpu.VMEM((len(halves) // 2, 2) + halves[0].shape, halves[0].dtype)


def side_scratch():
    return pltpu.VMEM((2, 16, 128), jnp.bfloat16)


def first(lists, q, own_rows, halves, latent, scale):
    tiles, rows, _ = q.shape
    f32 = jnp.float32
    args = (lists, q, own_rows, *halves)
    return pl.pallas_call(
        functools.partial(first_kernel, pieces=len(halves), scale=scale),
        name="first",
        out_shape=(
            jax.ShapeDtypeStruct((tiles, rows, 128), f32),
            jax.ShapeDtypeStruct((tiles, rows, 128), f32),
            jax.ShapeDtypeStruct((tiles, rows, latent), f32),
        ),
        in_specs=[sspec()] + [vspec()] * (len(args) - 1),
        out_specs=(vspec(),) * 3,
        scratch_shapes=[side_scratch()],
        compiler_params=params(16),
        cost_estimate=cost(5e9, 2e7),
    )(*args)


def stage_kernel(list_ref, q_ref, *refs, pieces, scale):
    sources = refs[:pieces]
    source, state, side_ref = refs[pieces : pieces + 3], refs[pieces + 3 : pieces + 6], refs[-1]
    for old, new in zip(source, state):
        new[...] = old[...]
    attend(list_ref, q_ref, sources, scale, state, side_ref, True)


def stage(lists, q, halves, state, scale):
    before = 2 + len(halves)
    args = (lists, q, *halves, *state)
    return pl.pallas_call(
        functools.partial(stage_kernel, pieces=len(halves), scale=scale),
        name="stage",
        out_shape=tuple(jax.ShapeDtypeStruct(x.shape, x.dtype) for x in state),
        in_specs=[sspec()] + [vspec()] * (len(args) - 1),
        out_specs=(vspec(),) * 3,
        scratch_shapes=[side_scratch()],
        input_output_aliases={before: 0, before + 1: 1, before + 2: 2},
        compiler_params=params(18),
        cost_estimate=cost(1e10, 2e7),
    )(*args)


def project(x, wo_ref, away, mine, list_ref, columns):
    room = list_ref.shape[1] - 3
    level, core = list_ref[0, room + 1], list_ref[0, room + 2]
    core = core if mine else 1 - core
    at = lax.rem(level + away, 4) * (2 * columns) + core * columns
    at = pl.multiple_of(at, 128)
    return dot(x, wo_ref[:, pl.ds(at, columns)]).astype(jnp.bfloat16)


def last_kernel(list_ref, q_ref, *refs, pieces, scale):
    halves = refs[:pieces]
    uv_ref, wo_ref = refs[pieces : pieces + 2]
    source = refs[pieces + 2 : pieces + 5]
    out_ref, mine_ref, other_ref = refs[pieces + 5 : pieces + 8]
    state, near, side_ref = refs[pieces + 8 : pieces + 11], refs[-2], refs[-1]
    gather(halves, near)
    for old, new in zip(source, state):
        new[...] = old[...]
    sources = [near.at[i] for i in range(near.shape[0])]
    attend(list_ref, q_ref, sources, scale, state, side_ref, True)
    for t in range(q_ref.shape[0]):
        total = jnp.sum(state[1][t], axis=1, keepdims=True)
        mixed = (state[2][t] / total).astype(jnp.bfloat16)
        for h in range(uv_ref.shape[0]):
            out_ref[t * TILE : (t + 1) * TILE, h * 128 : (h + 1) * 128] = dot(
                mixed[h * TILE : (h + 1) * TILE], uv_ref[h]
            ).astype(jnp.bfloat16)
    columns = mine_ref.shape[1]
    x = out_ref[...]
    other_ref[...] = project(x, wo_ref, 2, False, list_ref, columns)
    mine_ref[...] = project(x, wo_ref, 2, True, list_ref, columns)


def last(lists, q, halves, w_uv, state, w_o, scale):
    tiles, _, _ = state[2].shape
    tokens = tiles * TILE
    columns = w_o.shape[1] // 8
    bf = jnp.bfloat16
    args = (lists, q, *halves, w_uv, w_o, *state)
    before = len(args) - 3
    outs = pl.pallas_call(
        functools.partial(last_kernel, pieces=len(halves), scale=scale),
        name="last",
        out_shape=(
            jax.ShapeDtypeStruct((tokens, w_o.shape[0]), bf),
            jax.ShapeDtypeStruct((tokens, columns), bf),
            jax.ShapeDtypeStruct((tokens, columns), bf),
        )
        + tuple(jax.ShapeDtypeStruct(x.shape, x.dtype) for x in state),
        in_specs=[sspec()] + [vspec()] * (len(args) - 1),
        out_specs=(vspec(),) * 6,
        input_output_aliases={before: 3, before + 1: 4, before + 2: 5},
        scratch_shapes=[near_scratch(halves), side_scratch()],
        compiler_params=params(16),
        cost_estimate=cost(8e9, 2e7),
    )(*args)
    return outs[:3]


def columns_kernel(list_ref, x_ref, wo_ref, *out_refs, parts):
    x = x_ref[...]
    for ref, (aways, mine) in zip(out_refs, parts):
        for i, away in enumerate(aways):
            ref[i] = project(x, wo_ref, away, mine, list_ref, ref.shape[2])


def columns_of(lists, head_out, w_o, parts):
    tokens = head_out.shape[0]
    columns = w_o.shape[1] // 8
    count = sum(len(aways) for aways, _ in parts)
    return pl.pallas_call(
        functools.partial(columns_kernel, parts=parts),
        name="columns",
        out_shape=tuple(
            jax.ShapeDtypeStruct((len(aways), tokens, columns), jnp.bfloat16) for aways, _ in parts
        ),
        in_specs=[sspec(), vspec(), vspec()],
        out_specs=(vspec(),) * len(parts),
        compiler_params=params(8),
        cost_estimate=cost(5e8 * count, 2e6 * count),
    )(lists, head_out, w_o)


def finish_kernel(mine_ref, other_ref, *refs):
    out_ref = refs[-1]
    half = refs[0].shape[0]
    f32 = jnp.float32
    for i in range(2):
        rows = pl.ds(i * half, half)
        total = mine_ref[0, rows].astype(f32) + other_ref[0, rows].astype(f32)
        for ref in refs[2 * i : 2 * i + 2]:
            total = total + ref[...].astype(f32)
        out_ref[rows] = total.astype(jnp.bfloat16)


def finish(mine, other, top, bottom):
    args = (mine, other, *top, *bottom)
    return pl.pallas_call(
        finish_kernel,
        name="finish",
        out_shape=jax.ShapeDtypeStruct(mine.shape[1:], jnp.bfloat16),
        in_specs=[vspec()] * len(args),
        out_specs=vspec(),
        compiler_params=params(8),
    )(*args)


def per_device(queries, own_latent, cache, block_list, offsets, tile_mask, w_uk, w_uv, w_o):
    seq = ("x", "y")
    seq_index = lax.axis_index(seq)
    spans_held = cache.shape[0]
    listed_count = block_list.shape[1]
    latent_full = cache.shape[2]
    latent = w_uk.shape[2]
    rope = latent_full - latent
    width = w_uk.shape[1] + rope
    scale = width ** (-0.5)

    shift = spans_held.bit_length() - 1
    assert spans_held == 1 << shift
    owners = block_list >> shift
    within = block_list & (spans_held - 1)
    position = jnp.arange(listed_count, dtype=jnp.int32)
    earlier = position[None, :] < position[:, None]
    same_owner = owners[:, :, None] == owners[:, None, :]
    ranking = jnp.sum(same_owner & earlier[None], axis=2)
    slot_ids = jnp.arange(MOST, dtype=jnp.int32)
    matches = (owners == seq_index)[:, :, None] & (ranking[:, :, None] == slot_ids[None, None, :])
    send_index = jnp.sum(jnp.where(matches, within[:, :, None], 0), axis=1)
    my_owners = lax.dynamic_index_in_dim(owners, seq_index, 0, keepdims=False)
    my_ranking = lax.dynamic_index_in_dim(ranking, seq_index, 0, keepdims=False)
    flat_slot = my_owners * MOST + my_ranking
    sent = send(send_index, cache)
    arrived = lax.all_to_all(sent, seq, split_axis=0, concat_axis=0, tiled=True)

    place = jnp.stack([lax.axis_index("z"), lax.axis_index("c")]).astype(jnp.int32)
    inverse = THETA ** (-jnp.arange(rope // 2, dtype=jnp.float32) * 2.0 / rope)
    angles = offsets[0].astype(jnp.float32)[:, None] * inverse[None, :]
    cosine = jnp.cos(angles)
    sine = jnp.sin(angles)
    cosines = jnp.concatenate([cosine, cosine], axis=1)
    sines = jnp.concatenate([-sine, sine], axis=1)
    q, lists = start(place, tile_mask[0], queries, w_uk)

    own = pick(
        flat_slot,
        lists,
        arrived,
        cosines,
        sines,
    )
    size = 4
    up = [(i, (i + 1) % size) for i in range(size)]
    down = [(i, (i - 1) % size) for i in range(size)]
    swap = [(0, 1), (1, 0)]

    def other_core(x):
        return lax.ppermute(x, "c", swap)

    def move(x, ways):
        return lax.ppermute(x, "z", ways)

    plus = move(own, up)
    minus = move(own, down)
    twin = other_core(own)
    state = first(lists, q, own_latent, [own, twin], latent, scale)
    low = move(plus[0], up)
    high = move(minus[1], down)
    pieces = [plus, minus]
    pieces = pieces + [other_core(x) for x in pieces]
    state = stage(lists, q, pieces, state, scale)
    halves = [low, high]
    halves = halves + [other_core(x) for x in halves]
    head_out, far_mine, far_other = last(lists, q, halves, w_uv, state, w_o, scale)

    bf = jnp.bfloat16
    f32 = jnp.float32

    def add(*terms):
        return functools.reduce(jnp.add, [x.astype(f32) for x in terms])

    h = far_mine.shape[0] // 2
    far_other = other_core(far_other)
    (others,) = columns_of(lists, head_out, w_o, (((1, 3), False),))
    others = other_core(others)
    far = add(far_mine, far_other).astype(bf)
    below = move(far[:h], up)
    above = move(far[h:], down)
    (mine,) = columns_of(lists, head_out, w_o, (((1, 3), True),))
    early_up = move(add(mine[0, h:], others[0, h:]).astype(bf), up)
    early_down = move(add(mine[1, :h], others[1, :h]).astype(bf), down)
    kept_other, kept_mine = columns_of(
        lists, head_out, w_o, (((0,), False), ((0,), True))
    )
    late_up = move(add(mine[0, :h], others[0, :h], below).astype(bf), up)
    late_down = move(add(mine[1, h:], others[1, h:], above).astype(bf), down)
    kept_other = other_core(kept_other)
    return finish(kept_mine, kept_other, (late_up, early_down), (early_up, late_down))


def solution(mesh):
    fine = Mesh(mesh.devices.reshape(4, 4, 4, 2), ("x", "y", "z", "c"))
    seq = ("x", "y")
    head = ("z", "c")
    placed = (
        P(seq, head),
        P(seq, None),
        P(seq, head, None),
        P(),
        P(seq, None),
        P(seq, None, None),
        P(head, None, None),
        P(head, None, None),
        P(head, None),
    )
    return jax.shard_map(
        per_device, mesh=fine, in_specs=placed, out_specs=P(seq, head), check_vma=False
    )
```
